512 devices in a mesh: wide: 128 (over z, y, core), narrow: 4 (over x).
Axes of the slice: x: 4, y: 8, z: 8, core: 2. Of those that a mesh axis runs over, the one named last changes fastest.
Arguments:
- mesh_latent: bfloat16 [32768, 512], P(('wide', 'narrow')), may hold values from -6 to 6
- mesh_edges: bfloat16 [262144, 512], P(('wide', 'narrow')), may hold values from -6 to 6
- grid_latent: bfloat16 [131072, 512], P(('wide', 'narrow')), may hold values from -6 to 6
- decoder_edges: bfloat16 [393216, 512], P(('wide', 'narrow')), may hold values from -6 to 6
- mesh_senders: int32 [32768, 8], P(('wide', 'narrow')), may hold values from 0 to 4351
- mesh_degree: int32 [32768], P(('wide', 'narrow')), may hold values from 1 to 8
- decoder_senders: int32 [131072, 3], P(('wide', 'narrow')), may hold values from 0 to 319
- mesh_send_rows: int32 [128, 4, 128, 32], P('wide', 'narrow'), may hold values from 0 to 255
- decoder_send_rows: int32 [128, 4, 2, 32], P('wide', 'narrow'), may hold values from 0 to 255
- proc_edge_in: bfloat16 [1536, 512], P('wide'), may hold values from -0.15625 to 0.15625
- proc_edge_out: bfloat16 [512, 512], P('wide'), may hold values from -0.25 to 0.25
- proc_node_in: bfloat16 [1024, 512], P('wide'), may hold values from -0.1875 to 0.1875
- proc_node_out: bfloat16 [512, 512], P('wide'), may hold values from -0.25 to 0.25
- dec_edge_in: bfloat16 [1536, 512], P('wide'), may hold values from -0.15625 to 0.15625
- dec_edge_out: bfloat16 [512, 512], P('wide'), may hold values from -0.25 to 0.25
- grid_node_in: bfloat16 [1024, 512], P('wide'), may hold values from -0.1875 to 0.1875
- grid_node_out: bfloat16 [512, 512], P('wide'), may hold values from -0.25 to 0.25
- output_head: bfloat16 [512, 227], P('wide'), may hold values from -0.25 to 0.25
Outputs:
- mesh_out: bfloat16 [32768, 512], P(('wide', 'narrow'))
- edge_out: bfloat16 [262144, 512], P(('wide', 'narrow'))
- grid_pred: float32 [131072, 227], P(('wide', 'narrow'))
The draws below stay inside these ranges and needn't reach their ends.
Inputs may be any that keep to these rules, and one draw needn't show every extreme that they name: `mesh_senders`: slots name rows of the device's sender table: below 256 its own patch, above it 32 rows supplied by each patch in turn. A mesh node's live edges are its first mesh_degree slots. `decoder_senders`: slots name rows of the device's decoder sender table: below 256 its own patch, then 32 rows from the previous patch and 32 rows from the next patch. `mesh_send_rows`: entry [p, n, q, k] is a row of patch p. `decoder_send_rows`: entry [p, n, j, k] is a row of patch p.
All inputs are finite; a program needn't handle non-finite values.
Results may differ from the reference program's by a relative error of at most 0.012.
Values may be sent and summed in bfloat16 or wider, within the bound.
No kernel may reach another device: no remote copies, remote signals or barrier semaphores. Data moves between devices by JAX's collectives and lax.ppermute only.
A program may use at most 64 MiB of HBM per device.

```python
import jax
import jax.numpy as jnp
from jax import lax

D = 512
C = 227
NODE_DEV = 64
GRID_DEV = 256
DEG = 8
DDEG = 3
SEND = 32
DSEND = 32
PEERS = 128
GROUP = 4
PATCH = 256
MESH = 32768
EDGES = 262144
GRID = 131072
DEDGES = 393216
SLOTS = 4352
DSLOTS = 320
N_WIDE = 128
N_NARROW = 4


def with_ends(drawn, rng, least, largest):
    longest = drawn.shape.index(max(drawn.shape))
    spots = []
    for shift in (0, 1):
        where = [jax.random.randint(jax.random.fold_in(rng, axis), (), 0, length) for axis, length in enumerate(drawn.shape)]
        where[longest] = (where[longest] + shift) % drawn.shape[longest]
        spots.append(tuple(where))
    return drawn.at[spots[0]].set(least).at[spots[1]].set(largest)


def block_levels(rng, shape, cuts, smallest, largest):
    def one(dim, shards_of):
        heights = jax.random.uniform(jax.random.fold_in(jax.random.fold_in(rng, 6), dim), (shards_of,), jnp.float32, smallest / len(cuts), largest / len(cuts))
        return jnp.repeat(jnp.exp(heights), shape[dim] // shards_of).reshape((-1,) + (1,) * (len(shape) - dim - 1))

    level = one(*cuts[0])
    for cut in cuts[1:]:
        level = level * one(*cut)
    return level


def noise(rng, shape, deviation, bound, split=(), held_as=jnp.bfloat16):
    array = jax.random.normal(rng, shape, jnp.float32) * deviation
    if len(split) > 0:
        array = block_levels(rng, shape, split, -0.22, 0.18) * array
    return jnp.clip(array, min=-bound, max=bound).astype(held_as)


def setup_inputs(seed: int = 0) -> dict:
    splits = jax.random.split(jax.random.key(seed), 19)
    return {
        "mesh_latent": noise(splits[0], (MESH, D), 1.0, 6.0, ((0, 512),)),
        "mesh_edges": noise(splits[1], (EDGES, D), 1.0, 6.0, ((0, 512),)),
        "grid_latent": noise(splits[2], (GRID, D), 1.0, 6.0, ((0, 512),)),
        "decoder_edges": noise(splits[3], (DEDGES, D), 1.0, 6.0, ((0, 512),)),
        "mesh_senders": with_ends(jax.random.randint(splits[4], (MESH, DEG), 0, SLOTS), jax.random.fold_in(splits[4], 1), 0, SLOTS - 1).astype(jnp.int32),
        "mesh_degree": with_ends(jax.random.randint(splits[5], (MESH,), 1, DEG + 1), jax.random.fold_in(splits[5], 1), 1, DEG).astype(jnp.int32),
        "decoder_senders": with_ends(jax.random.randint(splits[6], (GRID, DDEG), 0, DSLOTS), jax.random.fold_in(splits[6], 1), 0, DSLOTS - 1).astype(jnp.int32),
        "mesh_send_rows": with_ends(jax.random.randint(splits[7], (PEERS, GROUP, PEERS, SEND), 0, PATCH), jax.random.fold_in(splits[7], 1), 0, PATCH - 1).astype(jnp.int32),
        "decoder_send_rows": with_ends(jax.random.randint(splits[8], (PEERS, GROUP, 2, DSEND), 0, PATCH), jax.random.fold_in(splits[8], 1), 0, PATCH - 1).astype(jnp.int32),
        "proc_edge_in": noise(splits[9], (3 * D, D), (3 * D) ** -0.5, 0.15625, ((0, 128),)),
        "proc_edge_out": noise(splits[10], (D, D), D ** -0.5, 0.25, ((0, 128),)),
        "proc_node_in": noise(splits[11], (2 * D, D), (2 * D) ** -0.5, 0.1875, ((0, 128),)),
        "proc_node_out": noise(splits[12], (D, D), D ** -0.5, 0.25, ((0, 128),)),
        "dec_edge_in": noise(splits[13], (3 * D, D), (3 * D) ** -0.5, 0.15625, ((0, 128),)),
        "dec_edge_out": noise(splits[14], (D, D), D ** -0.5, 0.25, ((0, 128),)),
        "grid_node_in": noise(splits[15], (2 * D, D), (2 * D) ** -0.5, 0.1875, ((0, 128),)),
        "grid_node_out": noise(splits[16], (D, D), D ** -0.5, 0.25, ((0, 128),)),
        "output_head": noise(splits[17], (D, C), D ** -0.5, 0.25, ((0, 128),)),
    }


def swish(values):
    return values * jax.nn.sigmoid(values)

def normalize(values):
    center = values - lax.optimization_barrier(jnp.mean(values, axis=-1, keepdims=True))
    spread = lax.optimization_barrier(jnp.mean(center * center, axis=-1, keepdims=True))
    return center * lax.rsqrt(spread + 1e-05)

def second_layer(hidden_pre, w_second):
    active = swish(hidden_pre).astype(jnp.bfloat16)
    return normalize(jnp.dot(active, w_second, preferred_element_type=jnp.float32))

def global_rows(slots, send_rows, width, per_device):
    patch = NODE_DEV * N_NARROW
    device = jnp.arange(slots.shape[0], dtype=jnp.int32) // per_device
    wide_index = (device // N_NARROW)[:, None]
    narrow_index = (device % N_NARROW)[:, None]
    halo = jnp.maximum(slots - patch, 0)
    peer = halo // width
    position = halo % width
    remote = send_rows[peer, narrow_index, wide_index, position]
    return jnp.where(slots < patch, wide_index * patch + slots, peer * patch + remote).astype(jnp.int32)

def decoder_rows(slots, send_rows):
    patch = NODE_DEV * N_NARROW
    device = jnp.arange(slots.shape[0], dtype=jnp.int32) // GRID_DEV
    wide_index = (device // N_NARROW)[:, None]
    narrow_index = (device % N_NARROW)[:, None]
    halo = jnp.maximum(slots - patch, 0)
    side = jnp.minimum(halo // DSEND, 1)
    position = halo % DSEND
    source = (wide_index - 1 + 2 * side + N_WIDE) % N_WIDE
    remote = send_rows[source, narrow_index, side, position]
    return jnp.where(slots < patch, wide_index * patch + slots, source * patch + remote).astype(jnp.int32)

def reference(mesh_latent, mesh_edges, grid_latent, decoder_edges, mesh_senders, mesh_degree, decoder_senders, mesh_send_rows, decoder_send_rows, proc_edge_in, proc_edge_out, proc_node_in, proc_node_out, dec_edge_in, dec_edge_out, grid_node_in, grid_node_out, output_head):
    devices = N_WIDE * N_NARROW
    send_term = jnp.dot(mesh_latent, proc_edge_in[D:2 * D], preferred_element_type=jnp.float32).astype(jnp.bfloat16)
    sender = global_rows(mesh_senders, mesh_send_rows, SEND, NODE_DEV)

    def processor_block(inputs):
        latent, edges, index, degree_live = inputs
        rows = jnp.take(send_term, index.reshape(-1), axis=0)
        receiver_term = jnp.dot(latent, proc_edge_in[2 * D:], preferred_element_type=jnp.float32)
        pre = jnp.dot(edges, proc_edge_in[:D], preferred_element_type=jnp.float32).reshape(-1, DEG, D)
        pre = pre + rows.reshape(-1, DEG, D) + receiver_term[:, None, :]
        updated = (edges + second_layer(pre.reshape(-1, D), proc_edge_out)).astype(jnp.bfloat16)
        live = (lax.broadcasted_iota(jnp.int32, (latent.shape[0], DEG), 1) < degree_live[:, None]).astype(jnp.float32)
        summed = lax.optimization_barrier(jnp.sum(updated.reshape(-1, DEG, D).astype(jnp.float32) * live[:, :, None], axis=1)).astype(jnp.bfloat16)
        node_pre = jnp.dot(latent, proc_node_in[:D], preferred_element_type=jnp.float32) + jnp.dot(summed, proc_node_in[D:], preferred_element_type=jnp.float32)
        new_latent = (latent + second_layer(node_pre, proc_node_out)).astype(jnp.bfloat16)
        return (new_latent, updated)
    mesh_out, edge_out = lax.map(processor_block, (mesh_latent.reshape(devices, NODE_DEV, D), mesh_edges.reshape(devices, NODE_DEV * DEG, D), sender.reshape(devices, NODE_DEV, DEG), mesh_degree.reshape(devices, NODE_DEV)))
    mesh_out = mesh_out.reshape(-1, D)
    edge_out = edge_out.reshape(-1, D)
    dsend_term = jnp.dot(mesh_out, dec_edge_in[D:2 * D], preferred_element_type=jnp.float32).astype(jnp.bfloat16)
    dsender = decoder_rows(decoder_senders, decoder_send_rows)

    def decoder_block(inputs):
        latent, edges, index = inputs
        rows = jnp.take(dsend_term, index.reshape(-1), axis=0)
        receiver_term = jnp.dot(latent, dec_edge_in[2 * D:], preferred_element_type=jnp.float32)
        pre = jnp.dot(edges, dec_edge_in[:D], preferred_element_type=jnp.float32).reshape(-1, DDEG, D)
        pre = pre + rows.reshape(-1, DDEG, D) + receiver_term[:, None, :]
        updated = (edges + second_layer(pre.reshape(-1, D), dec_edge_out)).astype(jnp.bfloat16)
        summed = lax.optimization_barrier(jnp.sum(updated.reshape(-1, DDEG, D).astype(jnp.float32), axis=1)).astype(jnp.bfloat16)
        node_pre = jnp.dot(latent, grid_node_in[:D], preferred_element_type=jnp.float32) + jnp.dot(summed, grid_node_in[D:], preferred_element_type=jnp.float32)
        new_grid = (latent + second_layer(node_pre, grid_node_out)).astype(jnp.bfloat16)
        return jnp.dot(new_grid, output_head, preferred_element_type=jnp.float32)
    grid_pred = lax.map(decoder_block, (grid_latent.reshape(devices, GRID_DEV, D), decoder_edges.reshape(devices, GRID_DEV * DDEG, D), dsender.reshape(devices, GRID_DEV, DDEG)))
    return (mesh_out, edge_out, grid_pred.reshape(-1, C))
```

```python
import jax
import jax.numpy as jnp
from jax import lax
from jax.experimental import pallas as pl
from jax.experimental.pallas import tpu as pltpu
from jax.sharding import PartitionSpec as P

BF16 = jnp.bfloat16
F32 = jnp.float32
CAPACITY = 192


def matmul(a, b):
    return jnp.dot(a, b, preferred_element_type=F32)


def second_layer(pre, w_second):
    active = (pre / (1.0 + jnp.exp(-pre))).astype(BF16)
    values = matmul(active, w_second)
    center = values - jnp.mean(values, axis=-1, keepdims=True)
    spread = jnp.mean(center * center, axis=-1, keepdims=True)
    return center * lax.rsqrt(spread + 1e-05)


def marks(hit):
    return jnp.where(hit, 1.0, 0.0).astype(BF16)


def selection(index, size):
    columns = lax.broadcasted_iota(jnp.int32, (index.shape[0], size), 1)
    return marks(index == columns)


def pack_kernel(*refs):
    *pieces, out, stage = refs
    stage[...] = jnp.zeros_like(stage)
    first = 0
    for piece in pieces:
        rows, columns = piece.shape
        stage[first : first + rows, 0:columns] = piece[...].astype(F32)
        first += rows
    out[...] = stage[...].astype(BF16)


def packed(pieces, rows, width):
    return pl.pallas_call(
        pack_kernel,
        out_shape=jax.ShapeDtypeStruct((rows, width), BF16),
        scratch_shapes=[pltpu.VMEM((rows, width), F32)],
        name="pack",
    )(*pieces)


def processor_kernel(
    place, live, got, extra, edges, near, latent, w_first, w_second, n_first, n_second, edge_out, mesh_out, messages
):
    step, steps = pl.program_id(0), pl.num_programs(0)
    width = edges.shape[1]
    rows = matmul(selection(place[...], got.shape[0]), got[...]) + extra[...].astype(F32)
    sent = matmul(rows.astype(BF16), w_first[width : 2 * width]).astype(BF16)
    receiver = matmul(near[...], w_first[2 * width :])
    count = receiver.shape[0]
    spread = jnp.broadcast_to(receiver[:, None, :], (count, edges.shape[0] // count, width))
    pre = matmul(edges[...], w_first[:width]) + sent.astype(F32) + spread.reshape(edges.shape)
    updated = (edges[...].astype(F32) + second_layer(pre, w_second[...])).astype(BF16)
    edge_out[...] = updated
    kept = (updated.astype(F32) * live[...]).reshape(spread.shape)
    messages[pl.ds(pl.multiple_of(step * count, count), count)] = jnp.sum(kept, axis=1).astype(BF16)

    @pl.when(step == steps - 1)
    def _():
        node_pre = matmul(latent[...], n_first[:width]) + matmul(messages[...], n_first[width:])
        mesh_out[...] = (latent[...].astype(F32) + second_layer(node_pre, n_second[...])).astype(BF16)


def processor(place, live, got, extra, edges, latent, w_first, w_second, n_first, n_second, steps=4):
    slots, width = edges.shape
    nodes = latent.shape[0]

    def tiles(array):
        return pl.BlockSpec((array.shape[0] // steps, array.shape[1]), lambda i: (i, 0))

    def whole(array):
        return pl.BlockSpec(array.shape, lambda i: (0, 0))

    return pl.pallas_call(
        processor_kernel,
        grid=(steps,),
        in_specs=[tiles(place), tiles(live), whole(got), tiles(extra), tiles(edges), tiles(latent), whole(latent)]
        + [whole(w) for w in (w_first, w_second, n_first, n_second)],
        out_specs=[tiles(edges), whole(latent)],
        out_shape=[jax.ShapeDtypeStruct(edges.shape, BF16), jax.ShapeDtypeStruct(latent.shape, BF16)],
        scratch_shapes=[pltpu.VMEM((nodes, width), BF16)],
        cost_estimate=pl.CostEstimate(flops=2_000_000_000, bytes_accessed=8_000_000, transcendentals=600_000),
        name="processor",
    )(place, live, got, extra, edges, latent, latent, w_first, w_second, n_first, n_second)


def decoder_kernel(
    named, index, near_a, near_b, edges, latent, w_first, w_second, n_first, n_second, head, out, sent
):
    width = edges.shape[1]

    @pl.when(pl.program_id(0) == 0)
    def _():
        columns = near_a.shape[0]
        table = matmul(selection(named[...], columns), near_a[...])
        table = table + matmul(selection(named[...] - columns, columns), near_b[...])
        sent[...] = matmul(table.astype(BF16), w_first[width : 2 * width]).astype(BF16)

    count, points = edges.shape[0], latent.shape[0]
    fanin = count // points
    offset = lax.broadcasted_iota(jnp.int32, (count, points), 0) - fanin * lax.broadcasted_iota(
        jnp.int32, (count, points), 1
    )
    onto = lax.broadcasted_iota(jnp.int32, (points, count), 1) - fanin * lax.broadcasted_iota(
        jnp.int32, (points, count), 0
    )
    receivers = matmul(marks((offset >= 0) & (offset < fanin)), latent[...]).astype(BF16)
    pre = matmul(edges[...], w_first[:width]) + matmul(receivers, w_first[2 * width :])
    pre = pre + matmul(selection(index[...], sent.shape[0]), sent[...])
    updated = (edges[...].astype(F32) + second_layer(pre, w_second[...])).astype(BF16)
    summed = matmul(marks((onto >= 0) & (onto < fanin)), updated).astype(BF16)
    point_pre = matmul(latent[...], n_first[:width]) + matmul(summed, n_first[width:])
    point_new = (latent[...].astype(F32) + second_layer(point_pre, n_second[...])).astype(BF16)
    out[...] = matmul(point_new, head[...])


def decoder(named, index, near_a, near_b, edges, latent, w_first, w_second, n_first, n_second, head, steps=2):
    width = edges.shape[1]

    def tiles(array):
        return pl.BlockSpec((array.shape[0] // steps, array.shape[1]), lambda i: (i, 0))

    def whole(array):
        return pl.BlockSpec(array.shape, lambda i: (0, 0))

    out = jax.ShapeDtypeStruct((latent.shape[0], head.shape[1]), F32)
    return pl.pallas_call(
        decoder_kernel,
        grid=(steps,),
        in_specs=[whole(named), tiles(index), whole(near_a), whole(near_b), tiles(edges), tiles(latent)]
        + [whole(w) for w in (w_first, w_second, n_first, n_second, head)],
        out_specs=tiles(out),
        out_shape=out,
        scratch_shapes=[pltpu.VMEM((named.shape[0], width), BF16)],
        cost_estimate=pl.CostEstimate(flops=3_000_000_000, bytes_accessed=8_000_000, transcendentals=1_000_000),
        name="decoder",
    )(named, index, near_a, near_b, edges, latent, w_first, w_second, n_first, n_second, head)


def exchanged(blocks, axis):
    return lax.all_to_all(blocks, axis, split_axis=0, concat_axis=0, tiled=True)


def passed_along(block, axis, distance):
    count = lax.axis_size(axis)
    return lax.ppermute(block, axis, [((i - distance) % count, i) for i in range(count)])


def one_hot(index, size):
    return (index[:, None] == lax.broadcasted_iota(jnp.int32, (1, size), 1)).astype(BF16)


def wanted_rows(senders, send_rows, nodes):
    peers, send = send_rows.shape
    group = lax.axis_size("narrow")
    patch = nodes * group
    slots = senders.reshape(-1)
    incoming = exchanged(send_rows, "wide")
    halo = jnp.maximum(slots - patch, 0)
    lists = matmul(one_hot(halo // send, peers), incoming.astype(BF16))
    column = lax.broadcasted_iota(jnp.int32, (1, send), 1)
    remote = jnp.sum(jnp.where((halo % send)[:, None] == column, lists, 0.0), axis=1)
    own = slots < patch
    row = jnp.where(own, slots, remote.astype(jnp.int32))
    source = jnp.where(own, lax.axis_index("wide"), halo // send)
    return row // nodes, source, row % nodes


def ranks_within(owner, group):
    mine = one_hot(owner, group)
    count = owner.shape[0]
    before = lax.broadcasted_iota(jnp.int32, (count, count), 0) > lax.broadcasted_iota(
        jnp.int32, (count, count), 1
    )
    earlier = matmul(before.astype(BF16), mine)
    rank = jnp.sum(earlier * mine.astype(F32), axis=1).astype(jnp.int32)
    most = jnp.max(jnp.sum(mine.astype(F32), axis=0))
    return rank, most


def requests(select, source, local, stride, capacity, most):
    group = lax.axis_size("narrow")
    asked = matmul(jnp.stack([source, local], axis=0).astype(BF16), select).astype(jnp.int32)
    ids = (asked[0] * stride + asked[1]).reshape(group, capacity)
    ids = jnp.pad(ids, ((0, 0), (0, -capacity % 128 + 128)))
    lane = lax.broadcasted_iota(jnp.int32, (1, ids.shape[1]), 1)
    here = exchanged(jnp.where(lane == capacity, most, ids), "narrow")
    return here[:, :capacity].reshape(-1), jnp.max(here[:, capacity])


def places(owner, rank, first, capacity):
    here = rank - first
    return jnp.where((here >= 0) & (here < capacity), owner * capacity + here, -1)


def rows_of(table, ids):
    return table.at[ids].get(mode="promise_in_bounds")


def delivered(found):
    width = found.shape[1]
    return exchanged(found.reshape(lax.axis_size("narrow"), -1, width), "narrow").reshape(-1, width)


def all_devices_max(value):
    copies = jnp.broadcast_to(value, (lax.axis_size("wide"), 8))
    return jnp.max(exchanged(copies, "wide"))


def two_patches(block, first):
    group, peers = lax.axis_size("narrow"), lax.axis_size("wide")
    count = group * peers
    members = [
        [(2 * group * k + first * group + j) % count for j in range(2 * group)] for k in range(peers // 2)
    ]
    copies = jnp.broadcast_to(block, (2 * group, *block.shape))
    got = lax.all_to_all(
        copies, ("wide", "narrow"), split_axis=0, concat_axis=0, axis_index_groups=members, tiled=True
    )
    return got.reshape(-1, block.shape[1])


def body(
    mesh_latent,
    mesh_edges,
    grid_latent,
    decoder_edges,
    mesh_senders,
    mesh_degree,
    decoder_senders,
    mesh_send_rows,
    decoder_send_rows,
    proc_edge_in,
    proc_edge_out,
    proc_node_in,
    proc_node_out,
    dec_edge_in,
    dec_edge_out,
    grid_node_in,
    grid_node_out,
    output_head,
):
    nodes, width = mesh_latent.shape
    degree = mesh_senders.shape[1]
    slots = nodes * degree
    channels = output_head.shape[1]
    pieces = (mesh_latent, proc_edge_in, proc_edge_out, proc_node_in, proc_node_out, output_head)
    pieces = pieces + (dec_edge_in, dec_edge_out, grid_node_in, grid_node_out)
    pack = packed(pieces, 2 * nodes, width)
    stride = pack.shape[0]
    table = lax.all_gather(pack, "wide", axis=0, tiled=True)

    def weight(gathered, first, count):
        parts = gathered.reshape(-1, stride, width)
        return parts[:, nodes + first : nodes + first + count].reshape(-1, width)

    owner, source, local = wanted_rows(mesh_senders, mesh_send_rows[0, 0], nodes)
    rank, most = ranks_within(owner, lax.axis_size("narrow"))
    group = lax.axis_size("narrow")
    place = places(owner, rank, 0, CAPACITY)
    ids, most = requests(one_hot(place, group * CAPACITY), source, local, stride, CAPACITY, most.astype(jnp.int32))
    most = all_devices_max(most)
    lists = decoder_send_rows[0, 0]
    odd = lax.axis_index("wide") % 2
    span = nodes * group
    named = jnp.concatenate(
        [
            odd * span + jnp.arange(span, dtype=jnp.int32),
            (1 - odd) * 2 * span + passed_along(lists[0], "wide", 1),
            (1 + 2 * odd) * span + passed_along(lists[1], "wide", -1),
        ]
    )
    live = lax.broadcasted_iota(jnp.int32, (nodes, degree), 1) < mesh_degree[:, None]
    place, live, named, index, ids = lax.optimization_barrier(
        (
            place.reshape(-1, 1),
            live.astype(F32).reshape(-1, 1),
            named.reshape(-1, 1),
            decoder_senders.reshape(-1, 1),
            ids,
        )
    )
    found = rows_of(table, ids)
    got = delivered(found)
    most, _ = lax.optimization_barrier((most, found))

    def fetch_rest():
        rest = slots - CAPACITY
        late = one_hot(places(owner, rank, CAPACITY, rest), group * rest)
        late_ids, _ = requests(late, source, local, stride, rest, most)
        return matmul(late, delivered(rows_of(table, late_ids))).astype(BF16)

    extra = lax.cond(most > CAPACITY, fetch_rest, lambda: jnp.zeros((slots, width), BF16))
    edge_out, mesh_out = processor(
        place,
        live,
        got,
        extra,
        mesh_edges,
        mesh_latent,
        weight(table, 0, 12),
        weight(table, 12, 4),
        weight(table, 16, 8),
        weight(table, 24, 4),
    )

    late_table, _ = lax.optimization_barrier((table, mesh_out))
    grid_pred = decoder(
        named,
        index,
        two_patches(mesh_out, 0),
        two_patches(mesh_out, 1),
        decoder_edges,
        grid_latent,
        weight(late_table, 32, 12),
        weight(late_table, 44, 4),
        weight(late_table, 48, 8),
        weight(late_table, 56, 4),
        weight(late_table, 28, 4)[:, :channels],
    )
    return (mesh_out, edge_out, grid_pred)


def solution(mesh):
    rows = P(("wide", "narrow"), None)
    lists = P("wide", "narrow", None, None)
    return jax.shard_map(
        body,
        mesh=mesh,
        in_specs=(rows,) * 5 + (P(("wide", "narrow")), rows, lists, lists) + (P("wide", None),) * 9,
        out_specs=(rows,) * 3,
        check_vma=False,
    )
```

```python
import jax
import jax.numpy as jnp
from jax import lax
from jax.experimental import pallas as pl
from jax.experimental.pallas import tpu as pltpu
from jax.sharding import PartitionSpec as P

BF16 = jnp.bfloat16
F32 = jnp.float32
CAPACITY = 176


def matmul(a, b):
    return jnp.dot(a, b, preferred_element_type=F32)


def second_layer(pre, w_second):
    active = (pre / (1.0 + jnp.exp(-pre))).astype(BF16)
    values = matmul(active, w_second)
    center = values - jnp.mean(values, axis=-1, keepdims=True)
    spread = jnp.mean(center * center, axis=-1, keepdims=True)
    return center * lax.rsqrt(spread + 1e-05)


def marks(hit):
    return jnp.where(hit, 1.0, 0.0).astype(BF16)


def selection(index, size):
    columns = lax.broadcasted_iota(jnp.int32, (index.shape[0], size), 1)
    return marks(index == columns)


def pack_kernel(*refs):
    *pieces, out, stage = refs
    stage[...] = jnp.zeros_like(stage)
    first = 0
    for piece in pieces:
        rows, columns = piece.shape
        stage[first : first + rows, 0:columns] = piece[...].astype(F32)
        first += rows
    out[...] = stage[...].astype(BF16)


def packed(pieces, rows, width):
    return pl.pallas_call(
        pack_kernel,
        out_shape=jax.ShapeDtypeStruct((rows, width), BF16),
        scratch_shapes=[pltpu.VMEM((rows, width), F32)],
        name="pack",
    )(*pieces)


def processor_kernel(
    place, live, got, extra, edges, near, latent, w_first, w_second, n_first, n_second, edge_out, mesh_out, copies, messages
):
    step, steps = pl.program_id(0), pl.num_programs(0)
    width = edges.shape[1]
    rows = matmul(selection(place[...], got.shape[0]), got[...]) + extra[...].astype(F32)
    sent = matmul(rows.astype(BF16), w_first[width : 2 * width]).astype(BF16)
    receiver = matmul(near[...], w_first[2 * width :])
    count = receiver.shape[0]
    spread = jnp.broadcast_to(receiver[:, None, :], (count, edges.shape[0] // count, width))
    pre = matmul(edges[...], w_first[:width]) + sent.astype(F32) + spread.reshape(edges.shape)
    updated = (edges[...].astype(F32) + second_layer(pre, w_second[...])).astype(BF16)
    edge_out[...] = updated
    kept = (updated.astype(F32) * live[...]).reshape(spread.shape)
    messages[pl.ds(pl.multiple_of(step * count, count), count)] = jnp.sum(kept, axis=1).astype(BF16)

    @pl.when(step == steps - 1)
    def _():
        node_pre = matmul(latent[...], n_first[:width]) + matmul(messages[...], n_first[width:])
        new = (latent[...].astype(F32) + second_layer(node_pre, n_second[...])).astype(BF16)
        mesh_out[...] = new
        for copy in range(copies.shape[0]):
            copies[copy] = new


def processor(place, live, got, extra, edges, latent, w_first, w_second, n_first, n_second, count, steps=2):
    slots, width = edges.shape
    nodes = latent.shape[0]

    def tiles(array):
        return pl.BlockSpec((array.shape[0] // steps, array.shape[1]), lambda i: (i, 0))

    def whole(array):
        return pl.BlockSpec(array.shape, lambda i: (0, 0))

    return pl.pallas_call(
        processor_kernel,
        grid=(steps,),
        in_specs=[tiles(place), tiles(live), whole(got), tiles(extra), tiles(edges), tiles(latent), whole(latent)]
        + [whole(w) for w in (w_first, w_second, n_first, n_second)],
        out_specs=[tiles(edges), whole(latent), pl.BlockSpec((count, *latent.shape), lambda i: (0, 0, 0))],
        out_shape=[jax.ShapeDtypeStruct(a, BF16) for a in (edges.shape, latent.shape, (count, *latent.shape))],
        scratch_shapes=[pltpu.VMEM((nodes, width), BF16)],
        cost_estimate=pl.CostEstimate(flops=2_000_000_000, bytes_accessed=8_000_000, transcendentals=600_000),
        name="processor",
    )(place, live, got, extra, edges, latent, latent, w_first, w_second, n_first, n_second)


def decoder_first_kernel(named, index, near, edges, latent, w_first, out, sent):
    width = edges.shape[1]

    @pl.when(pl.program_id(0) == 0)
    def _():
        table = matmul(selection(named[...], near.shape[0]), near[...])
        sent[...] = matmul(table.astype(BF16), w_first[width : 2 * width]).astype(BF16)

    count, points = edges.shape[0], latent.shape[0]
    fanin = count // points
    offset = lax.broadcasted_iota(jnp.int32, (count, points), 0) - fanin * lax.broadcasted_iota(
        jnp.int32, (count, points), 1
    )
    receivers = matmul(marks((offset >= 0) & (offset < fanin)), latent[...]).astype(BF16)
    pre = matmul(edges[...], w_first[:width]) + matmul(receivers, w_first[2 * width :])
    out[...] = pre + matmul(selection(index[...], sent.shape[0]), sent[...])


def tiles_of(array, steps):
    return pl.BlockSpec((array.shape[0] // steps, array.shape[1]), lambda i: (i, 0))


def whole_of(array):
    return pl.BlockSpec(array.shape, lambda i: (0, 0))


def decoder_first(named, index, near, edges, latent, w_first, steps=2):
    out = jax.ShapeDtypeStruct(edges.shape, F32)
    return pl.pallas_call(
        decoder_first_kernel,
        grid=(steps,),
        in_specs=[
            whole_of(named),
            tiles_of(index, steps),
            whole_of(near),
            tiles_of(edges, steps),
            tiles_of(latent, steps),
            whole_of(w_first),
        ],
        out_specs=tiles_of(out, steps),
        out_shape=out,
        scratch_shapes=[pltpu.VMEM((named.shape[0], edges.shape[1]), BF16)],
        cost_estimate=pl.CostEstimate(flops=2_000_000_000, bytes_accessed=6_000_000, transcendentals=0),
        name="decoder_first",
    )(named, index, near, edges, latent, w_first)


def decoder_second_kernel(
    start, index, far, first, edges, latent, w_send, w_second, n_first, n_second, head, out
):
    count, width = edges.shape
    points = latent.shape[0]
    fanin = count // points
    onto = lax.broadcasted_iota(jnp.int32, (points, count), 1) - fanin * lax.broadcasted_iota(
        jnp.int32, (points, count), 0
    )
    sent = matmul(far[...], w_send[...]).astype(BF16)
    pre = first[...] + matmul(selection(index[...] - start[0], sent.shape[0]), sent)
    updated = (edges[...].astype(F32) + second_layer(pre, w_second[...])).astype(BF16)
    summed = matmul(marks((onto >= 0) & (onto < fanin)), updated).astype(BF16)
    point_pre = matmul(latent[...], n_first[:width]) + matmul(summed, n_first[width:])
    point_new = (latent[...].astype(F32) + second_layer(point_pre, n_second[...])).astype(BF16)
    out[...] = lax.dot_general(
        head[...], point_new, (((0,), (1,)), ((), ())), preferred_element_type=F32
    )


def decoder_second(start, index, far, first, edges, latent, w_first, w_second, n_first, n_second, head, steps=2):
    points, width = latent.shape
    channels = head.shape[1]
    send = pl.BlockSpec((width, width), lambda i: (1, 0))
    return pl.pallas_call(
        decoder_second_kernel,
        grid=(steps,),
        in_specs=[
            pl.BlockSpec(memory_space=pltpu.SMEM),
            tiles_of(index, steps),
            whole_of(far),
            tiles_of(first, steps),
            tiles_of(edges, steps),
            tiles_of(latent, steps),
            send,
        ]
        + [whole_of(w) for w in (w_second, n_first, n_second, head)],
        out_specs=pl.BlockSpec((channels, points // steps), lambda i: (0, i)),
        out_shape=jax.ShapeDtypeStruct((channels, points), F32),
        cost_estimate=pl.CostEstimate(flops=2_000_000_000, bytes_accessed=6_000_000, transcendentals=1_000_000),
        name="decoder_second",
    )(start, index, far, first, edges, latent, w_first, w_second, n_first, n_second, head)


def exchanged(blocks, axis):
    return lax.all_to_all(blocks, axis, split_axis=0, concat_axis=0, tiled=True)


def swapped(block, axis, first):
    count = lax.axis_size(axis)
    pairs = [((first + i) % count, (first + (i ^ 1)) % count) for i in range(count)]
    return lax.ppermute(block, axis, pairs)


def one_hot(index, size):
    return (index[:, None] == lax.broadcasted_iota(jnp.int32, (1, size), 1)).astype(BF16)


def wanted_rows(senders, send_rows, nodes):
    peers, send = send_rows.shape
    group = lax.axis_size("narrow")
    patch = nodes * group
    slots = senders.reshape(-1)
    incoming = exchanged(send_rows, "wide")
    halo = jnp.maximum(slots - patch, 0)
    lists = matmul(one_hot(halo // send, peers), incoming.astype(BF16))
    column = lax.broadcasted_iota(jnp.int32, (1, send), 1)
    remote = jnp.sum(jnp.where((halo % send)[:, None] == column, lists, 0.0), axis=1)
    own = slots < patch
    row = jnp.where(own, slots, remote.astype(jnp.int32))
    source = jnp.where(own, lax.axis_index("wide"), halo // send)
    return row // nodes, source, row % nodes


def ranks_within(owner, group):
    mine = one_hot(owner, group)
    count = owner.shape[0]
    before = lax.broadcasted_iota(jnp.int32, (count, count), 0) > lax.broadcasted_iota(
        jnp.int32, (count, count), 1
    )
    earlier = matmul(before.astype(BF16), mine)
    rank = jnp.sum(earlier * mine.astype(F32), axis=1).astype(jnp.int32)
    most = jnp.max(jnp.sum(mine.astype(F32), axis=0))
    return rank, most


def requests(select, source, local, stride, capacity, most):
    group = lax.axis_size("narrow")
    asked = matmul(jnp.stack([source, local], axis=0).astype(BF16), select).astype(jnp.int32)
    ids = (asked[0] * stride + asked[1]).reshape(group, capacity)
    ids = jnp.pad(ids, ((0, 0), (0, -capacity % 128 + 128)))
    lane = lax.broadcasted_iota(jnp.int32, (1, ids.shape[1]), 1)
    here = exchanged(jnp.where(lane == capacity, most, ids), "narrow")
    return here[:, :capacity].reshape(-1), jnp.max(here[:, capacity])


def places(owner, rank, first, capacity):
    here = rank - first
    return jnp.where((here >= 0) & (here < capacity), owner * capacity + here, -1)


def rows_of(table, ids):
    return table.at[ids].get(mode="promise_in_bounds")


def delivered(found):
    width = found.shape[1]
    return exchanged(found.reshape(lax.axis_size("narrow"), -1, width), "narrow").reshape(-1, width)


def all_devices_max(value):
    copies = jnp.broadcast_to(value, (lax.axis_size("wide"), 8))
    return jnp.max(exchanged(copies, "wide"))


def two_patches(copies):
    group = copies.shape[0]
    count = lax.axis_size("narrow") * lax.axis_size("wide")
    members = [list(range(first, first + group)) for first in range(0, count, group)]
    got = lax.all_to_all(
        copies, ("wide", "narrow"), split_axis=0, concat_axis=0, axis_index_groups=members, tiled=True
    )
    return got.reshape(-1, copies.shape[2])


def body(
    mesh_latent,
    mesh_edges,
    grid_latent,
    decoder_edges,
    mesh_senders,
    mesh_degree,
    decoder_senders,
    mesh_send_rows,
    decoder_send_rows,
    proc_edge_in,
    proc_edge_out,
    proc_node_in,
    proc_node_out,
    dec_edge_in,
    dec_edge_out,
    grid_node_in,
    grid_node_out,
    output_head,
):
    nodes, width = mesh_latent.shape
    degree = mesh_senders.shape[1]
    slots = nodes * degree
    channels = output_head.shape[1]
    pieces = (mesh_latent, proc_edge_in, proc_edge_out, proc_node_in, proc_node_out, output_head)
    pieces = pieces + (dec_edge_in, dec_edge_out, grid_node_in, grid_node_out)
    pack = packed(pieces, 2 * nodes, width)
    stride = pack.shape[0]
    table = lax.all_gather(pack, "wide", axis=0, tiled=True)

    def weight(gathered, first, count):
        parts = gathered.reshape(-1, stride, width)
        return parts[:, nodes + first : nodes + first + count].reshape(-1, width)

    owner, source, local = wanted_rows(mesh_senders, mesh_send_rows[0, 0], nodes)
    rank, most = ranks_within(owner, lax.axis_size("narrow"))
    group = lax.axis_size("narrow")
    place = places(owner, rank, 0, CAPACITY)
    ids, most = requests(one_hot(place, group * CAPACITY), source, local, stride, CAPACITY, most.astype(jnp.int32))
    most = all_devices_max(most)
    lists = decoder_send_rows[0, 0]
    odd = lax.axis_index("wide") % 2
    span = nodes * group
    after, before = lists[0], lists[1]
    beside = swapped(jnp.where(odd == 1, before, after), "wide", 0) + (1 - odd) * span
    outside = jnp.where(odd == 1, after, before) + odd * span
    own = odd * span + jnp.arange(span, dtype=jnp.int32)
    nowhere = jnp.full(beside.shape, -1, jnp.int32)
    named = jnp.concatenate(
        [own, jnp.where(odd == 1, beside, nowhere), jnp.where(odd == 1, nowhere, beside)]
    )
    start = (span + odd * beside.shape[0]).reshape(1)
    live = lax.broadcasted_iota(jnp.int32, (nodes, degree), 1) < mesh_degree[:, None]
    place, live, named, index, outside, start, ids = lax.optimization_barrier(
        (
            place.reshape(-1, 1),
            live.astype(F32).reshape(-1, 1),
            named.reshape(-1, 1),
            decoder_senders.reshape(-1, 1),
            outside,
            start,
            ids,
        )
    )
    found = rows_of(table, ids)
    got = delivered(found)
    most, _ = lax.optimization_barrier((most, found))

    def fetch_rest():
        rest = slots - CAPACITY
        late = one_hot(places(owner, rank, CAPACITY, rest), group * rest)
        late_ids, _ = requests(late, source, local, stride, rest, most)
        return matmul(late, delivered(rows_of(table, late_ids))).astype(BF16)

    extra = lax.cond(most > CAPACITY, fetch_rest, lambda: jnp.zeros((slots, width), BF16))
    edge_out, mesh_out, copies = processor(
        place,
        live,
        got,
        extra,
        mesh_edges,
        mesh_latent,
        weight(table, 0, 12),
        weight(table, 12, 4),
        weight(table, 16, 8),
        weight(table, 24, 4),
        2 * group,
    )

    late_table, _ = lax.optimization_barrier((table, mesh_out))
    near = two_patches(copies)
    far = swapped(matmul(one_hot(outside, near.shape[0]), near).astype(BF16), "wide", 1)
    de_first = weight(late_table, 32, 12)
    first = decoder_first(named, index, near, decoder_edges, grid_latent, de_first)
    grid_pred = decoder_second(
        start,
        index,
        far,
        first,
        decoder_edges,
        grid_latent,
        de_first,
        weight(late_table, 44, 4),
        weight(late_table, 48, 8),
        weight(late_table, 56, 4),
        weight(late_table, 28, 4)[:, :channels],
    ).T
    return (mesh_out, edge_out, grid_pred)


def solution(mesh):
    rows = P(("wide", "narrow"), None)
    lists = P("wide", "narrow", None, None)
    return jax.shard_map(
        body,
        mesh=mesh,
        in_specs=(rows,) * 5 + (P(("wide", "narrow")), rows, lists, lists) + (P("wide", None),) * 9,
        out_specs=(rows,) * 3,
        check_vma=False,
    )
```

```python
import jax
import jax.numpy as jnp
from jax import lax
from jax.experimental import pallas as pl
from jax.experimental.pallas import tpu as pltpu
from jax.sharding import PartitionSpec as P

BF16 = jnp.bfloat16
F32 = jnp.float32
CAPACITY = 176


def matmul(a, b):
    return jnp.dot(a, b, preferred_element_type=F32)


def second_layer(pre, w_second):
    active = (pre / (1.0 + jnp.exp(-pre))).astype(BF16)
    values = matmul(active, w_second)
    center = values - jnp.mean(values, axis=-1, keepdims=True)
    spread = jnp.mean(center * center, axis=-1, keepdims=True)
    return center * lax.rsqrt(spread + 1e-05)


def marks(hit):
    return jnp.where(hit, 1.0, 0.0).astype(BF16)


def selection(index, size):
    columns = lax.broadcasted_iota(jnp.int32, (index.shape[0], size), 1)
    return marks(index == columns)


def pack_kernel(*refs):
    *pieces, out, stage = refs
    stage[...] = jnp.zeros_like(stage)
    first = 0
    for piece in pieces:
        rows, columns = piece.shape
        stage[first : first + rows, 0:columns] = piece[...].astype(F32)
        first += rows
    out[...] = stage[...].astype(BF16)


def packed(pieces, rows, width):
    return pl.pallas_call(
        pack_kernel,
        out_shape=jax.ShapeDtypeStruct((rows, width), BF16),
        scratch_shapes=[pltpu.VMEM((rows, width), F32)],
        name="pack",
    )(*pieces)


def rows_in(gathered, first, rows):
    shards, _, width = gathered.shape
    count = rows // shards
    return pl.BlockSpec((shards, count, width), lambda *_: (0, first // count, 0))


def gather_kernel(ids, place, table, out, stage, sems):
    halves = sems.shape[0]
    count, block, width = stage.shape
    share = count // halves

    for half in range(halves):

        def begin(i, carry, half=half):
            row = half * share + i
            pltpu.make_async_copy(table.at[ids[row]], stage.at[row], sems.at[half]).start()
            return carry

        lax.fori_loop(0, share, begin, 0, unroll=8)

    batch = 256 // block
    column = lax.broadcasted_iota(jnp.int32, (batch, batch * block), 1)
    first = block * lax.broadcasted_iota(jnp.int32, (batch, batch * block), 0)
    for half in range(halves):
        mine = pl.ds(half * share, share)
        pltpu.make_async_copy(table.at[pl.ds(0, share)], stage.at[mine], sems.at[half]).wait()
        for k in range(share // batch):
            rows = pl.ds(half * share + k * batch, batch)
            pick = marks(column == first + place[rows])
            out[rows] = matmul(pick, stage[rows].reshape(batch * block, width)).astype(BF16)


def rows_of_blocks(table, ids, block=8, halves=2):
    count, width = ids.shape[0], table.shape[1]
    return pl.pallas_call(
        gather_kernel,
        in_specs=[
            pl.BlockSpec(memory_space=pltpu.SMEM),
            pl.BlockSpec(memory_space=pltpu.VMEM),
            pl.BlockSpec(memory_space=pl.ANY),
        ],
        out_specs=pl.BlockSpec(memory_space=pltpu.VMEM),
        out_shape=jax.ShapeDtypeStruct((count, width), BF16),
        scratch_shapes=[pltpu.VMEM((count, block, width), BF16), pltpu.SemaphoreType.DMA((halves,))],
        cost_estimate=pl.CostEstimate(flops=1_000_000_000, bytes_accessed=6_000_000, transcendentals=0),
        name="rows",
    )(ids // block, (ids % block).reshape(-1, 1), table.reshape(-1, block, width))


def processor_kernel(
    place, live, got, extra, edges, near, latent, w_first, w_second, n_first, n_second, edge_out, mesh_out, copies, messages
):
    step, steps = pl.program_id(0), pl.num_programs(0)
    width = edges.shape[1]
    rows = matmul(selection(place[...], got.shape[0]), got[...]) + extra[...].astype(F32)
    sent = matmul(rows.astype(BF16), w_first[width : 2 * width]).astype(BF16)
    receiver = matmul(near[...], w_first[2 * width :])
    count = receiver.shape[0]
    spread = jnp.broadcast_to(receiver[:, None, :], (count, edges.shape[0] // count, width))
    pre = matmul(edges[...], w_first[:width]) + sent.astype(F32) + spread.reshape(edges.shape)
    updated = (edges[...].astype(F32) + second_layer(pre, w_second[...])).astype(BF16)
    edge_out[...] = updated
    kept = (updated.astype(F32) * live[...]).reshape(spread.shape)
    messages[pl.ds(pl.multiple_of(step * count, count), count)] = jnp.sum(kept, axis=1).astype(BF16)

    @pl.when(step == steps - 1)
    def _():
        inner = n_first[...].reshape(2 * width, width)
        node_pre = matmul(latent[...], inner[:width]) + matmul(messages[...], inner[width:])
        new = (latent[...].astype(F32) + second_layer(node_pre, n_second[...])).astype(BF16)
        mesh_out[...] = new
        for copy in range(copies.shape[0]):
            copies[copy] = new


def processor(place, live, got, extra, edges, latent, w_first, w_second, n_first, n_at, n_second, count, steps=2):
    slots, width = edges.shape
    nodes = latent.shape[0]

    def tiles(array):
        return pl.BlockSpec((array.shape[0] // steps, array.shape[1]), lambda i: (i, 0))

    def whole(array):
        return pl.BlockSpec(array.shape, lambda i: (0, 0))

    return pl.pallas_call(
        processor_kernel,
        grid=(steps,),
        in_specs=[tiles(place), tiles(live), whole(got), tiles(extra), tiles(edges), tiles(latent), whole(latent)]
        + [whole(w_first), whole(w_second), rows_in(n_first, n_at, 2 * width), whole(n_second)],
        out_specs=[tiles(edges), whole(latent), pl.BlockSpec((count, *latent.shape), lambda i: (0, 0, 0))],
        out_shape=[jax.ShapeDtypeStruct(a, BF16) for a in (edges.shape, latent.shape, (count, *latent.shape))],
        scratch_shapes=[pltpu.VMEM((nodes, width), BF16)],
        cost_estimate=pl.CostEstimate(flops=2_000_000_000, bytes_accessed=8_000_000, transcendentals=600_000),
        name="processor",
    )(place, live, got, extra, edges, latent, latent, w_first, w_second, n_first, n_second)


def decoder_first_kernel(named, index, near, edges, latent, w_first, out, sent):
    width = edges.shape[1]

    @pl.when(pl.program_id(0) == 0)
    def _():
        table = matmul(selection(named[...], near.shape[0]), near[...])
        sent[...] = matmul(table.astype(BF16), w_first[width : 2 * width]).astype(BF16)

    count, points = edges.shape[0], latent.shape[0]
    fanin = count // points
    offset = lax.broadcasted_iota(jnp.int32, (count, points), 0) - fanin * lax.broadcasted_iota(
        jnp.int32, (count, points), 1
    )
    receivers = matmul(marks((offset >= 0) & (offset < fanin)), latent[...]).astype(BF16)
    pre = matmul(edges[...], w_first[:width]) + matmul(receivers, w_first[2 * width :])
    out[...] = pre + matmul(selection(index[...], sent.shape[0]), sent[...])


def tiles_of(array, steps):
    return pl.BlockSpec((array.shape[0] // steps, array.shape[1]), lambda i: (i, 0))


def whole_of(array):
    return pl.BlockSpec(array.shape, lambda i: (0, 0))


def decoder_first(named, index, near, edges, latent, w_first, steps=2):
    out = jax.ShapeDtypeStruct(edges.shape, F32)
    return pl.pallas_call(
        decoder_first_kernel,
        grid=(steps,),
        in_specs=[
            whole_of(named),
            tiles_of(index, steps),
            whole_of(near),
            tiles_of(edges, steps),
            tiles_of(latent, steps),
            whole_of(w_first),
        ],
        out_specs=tiles_of(out, steps),
        out_shape=out,
        scratch_shapes=[pltpu.VMEM((named.shape[0], edges.shape[1]), BF16)],
        cost_estimate=pl.CostEstimate(flops=2_000_000_000, bytes_accessed=6_000_000, transcendentals=0),
        name="decoder_first",
    )(named, index, near, edges, latent, w_first)


def decoder_second_kernel(
    start, index, far, first, edges, latent, w_send, w_second, n_first, n_second, head, out
):
    count, width = edges.shape
    points = latent.shape[0]
    fanin = count // points
    onto = lax.broadcasted_iota(jnp.int32, (points, count), 1) - fanin * lax.broadcasted_iota(
        jnp.int32, (points, count), 0
    )
    sent = matmul(far[...], w_send[...]).astype(BF16)
    pre = first[...] + matmul(selection(index[...] - start[0], sent.shape[0]), sent)
    updated = (edges[...].astype(F32) + second_layer(pre, w_second[...])).astype(BF16)
    summed = matmul(marks((onto >= 0) & (onto < fanin)), updated).astype(BF16)
    inner = n_first[...].reshape(2 * width, width)
    point_pre = matmul(latent[...], inner[:width]) + matmul(summed, inner[width:])
    point_new = (latent[...].astype(F32) + second_layer(point_pre, n_second[...])).astype(BF16)
    out[...] = lax.dot_general(
        head[...], point_new, (((0,), (1,)), ((), ())), preferred_element_type=F32
    )


def decoder_second(start, index, far, first, edges, latent, w_first, w_second, n_first, n_at, n_second, head, steps=2):
    points, width = latent.shape
    channels = head.shape[1]
    send = pl.BlockSpec((width, width), lambda i: (1, 0))
    return pl.pallas_call(
        decoder_second_kernel,
        grid=(steps,),
        in_specs=[
            pl.BlockSpec(memory_space=pltpu.SMEM),
            tiles_of(index, steps),
            whole_of(far),
            tiles_of(first, steps),
            tiles_of(edges, steps),
            tiles_of(latent, steps),
            send,
        ]
        + [whole_of(w_second), rows_in(n_first, n_at, 2 * width), whole_of(n_second), whole_of(head)],
        out_specs=pl.BlockSpec((channels, points // steps), lambda i: (0, i)),
        out_shape=jax.ShapeDtypeStruct((channels, points), F32),
        cost_estimate=pl.CostEstimate(flops=2_000_000_000, bytes_accessed=6_000_000, transcendentals=1_000_000),
        name="decoder_second",
    )(start, index, far, first, edges, latent, w_first, w_second, n_first, n_second, head)


def exchanged(blocks, axis):
    return lax.all_to_all(blocks, axis, split_axis=0, concat_axis=0, tiled=True)


def swapped(block, axis, first):
    count = lax.axis_size(axis)
    pairs = [((first + i) % count, (first + (i ^ 1)) % count) for i in range(count)]
    return lax.ppermute(block, axis, pairs)


def one_hot(index, size):
    return (index[:, None] == lax.broadcasted_iota(jnp.int32, (1, size), 1)).astype(BF16)


def wanted_rows(senders, send_rows, nodes):
    peers, send = send_rows.shape
    group = lax.axis_size("narrow")
    patch = nodes * group
    slots = senders.reshape(-1)
    incoming = exchanged(send_rows, "wide")
    halo = jnp.maximum(slots - patch, 0)
    lists = matmul(one_hot(halo // send, peers), incoming.astype(BF16))
    column = lax.broadcasted_iota(jnp.int32, (1, send), 1)
    remote = jnp.sum(jnp.where((halo % send)[:, None] == column, lists, 0.0), axis=1)
    own = slots < patch
    row = jnp.where(own, slots, remote.astype(jnp.int32))
    source = jnp.where(own, lax.axis_index("wide"), halo // send)
    return row // nodes, source, row % nodes


def ranks_within(owner, group):
    mine = one_hot(owner, group)
    count = owner.shape[0]
    before = lax.broadcasted_iota(jnp.int32, (count, count), 0) > lax.broadcasted_iota(
        jnp.int32, (count, count), 1
    )
    earlier = matmul(before.astype(BF16), mine)
    rank = jnp.sum(earlier * mine.astype(F32), axis=1).astype(jnp.int32)
    most = jnp.max(jnp.sum(mine.astype(F32), axis=0))
    return rank, most


def requests(select, source, local, stride, capacity, most):
    group = lax.axis_size("narrow")
    asked = matmul(jnp.stack([source, local], axis=0).astype(BF16), select).astype(jnp.int32)
    ids = (asked[0] * stride + asked[1]).reshape(group, capacity)
    ids = jnp.pad(ids, ((0, 0), (0, -capacity % 128 + 128)))
    lane = lax.broadcasted_iota(jnp.int32, (1, ids.shape[1]), 1)
    here = exchanged(jnp.where(lane == capacity, most, ids), "narrow")
    return here[:, :capacity].reshape(-1), jnp.max(here[:, capacity])


def places(owner, rank, first, capacity):
    here = rank - first
    return jnp.where((here >= 0) & (here < capacity), owner * capacity + here, -1)


def rows_of(table, ids):
    return table.at[ids].get(mode="promise_in_bounds")


def delivered(found):
    width = found.shape[1]
    return exchanged(found.reshape(lax.axis_size("narrow"), -1, width), "narrow").reshape(-1, width)


def all_devices_max(value):
    copies = jnp.broadcast_to(value, (lax.axis_size("wide"), 8))
    return jnp.max(exchanged(copies, "wide"))


def two_patches(copies):
    group = copies.shape[0]
    count = lax.axis_size("narrow") * lax.axis_size("wide")
    members = [list(range(first, first + group)) for first in range(0, count, group)]
    got = lax.all_to_all(
        copies, ("wide", "narrow"), split_axis=0, concat_axis=0, axis_index_groups=members, tiled=True
    )
    return got.reshape(-1, copies.shape[2])


def body(
    mesh_latent,
    mesh_edges,
    grid_latent,
    decoder_edges,
    mesh_senders,
    mesh_degree,
    decoder_senders,
    mesh_send_rows,
    decoder_send_rows,
    proc_edge_in,
    proc_edge_out,
    proc_node_in,
    proc_node_out,
    dec_edge_in,
    dec_edge_out,
    grid_node_in,
    grid_node_out,
    output_head,
):
    nodes, width = mesh_latent.shape
    degree = mesh_senders.shape[1]
    slots = nodes * degree
    channels = output_head.shape[1]
    pieces = (mesh_latent, proc_edge_in, proc_edge_out, proc_node_in, proc_node_out, output_head)
    pieces = pieces + (dec_edge_in, dec_edge_out, grid_node_in, grid_node_out)
    pack = packed(pieces, 2 * nodes, width)
    stride = pack.shape[0]
    table = lax.all_gather(pack, "wide", axis=0, tiled=True)

    def weight(gathered, first, count):
        parts = gathered.reshape(-1, stride, width)
        return parts[:, nodes + first : nodes + first + count].reshape(-1, width)

    owner, source, local = wanted_rows(mesh_senders, mesh_send_rows[0, 0], nodes)
    rank, most = ranks_within(owner, lax.axis_size("narrow"))
    group = lax.axis_size("narrow")
    place = places(owner, rank, 0, CAPACITY)
    ids, most = requests(one_hot(place, group * CAPACITY), source, local, stride, CAPACITY, most.astype(jnp.int32))
    most = all_devices_max(most)
    lists = decoder_send_rows[0, 0]
    odd = lax.axis_index("wide") % 2
    span = nodes * group
    after, before = lists[0], lists[1]
    beside = swapped(jnp.where(odd == 1, before, after), "wide", 0) + (1 - odd) * span
    outside = jnp.where(odd == 1, after, before) + odd * span
    own = odd * span + jnp.arange(span, dtype=jnp.int32)
    nowhere = jnp.full(beside.shape, -1, jnp.int32)
    named = jnp.concatenate(
        [own, jnp.where(odd == 1, beside, nowhere), jnp.where(odd == 1, nowhere, beside)]
    )
    start = (span + odd * beside.shape[0]).reshape(1)
    live = lax.broadcasted_iota(jnp.int32, (nodes, degree), 1) < mesh_degree[:, None]
    place, live, named, index, outside, start, ids = lax.optimization_barrier(
        (
            place.reshape(-1, 1),
            live.astype(F32).reshape(-1, 1),
            named.reshape(-1, 1),
            decoder_senders.reshape(-1, 1),
            outside,
            start,
            ids,
        )
    )
    found = rows_of_blocks(table, ids)
    got = delivered(found)
    most, _ = lax.optimization_barrier((most, found))

    def fetch_rest():
        rest = slots - CAPACITY
        late = one_hot(places(owner, rank, CAPACITY, rest), group * rest)
        late_ids, _ = requests(late, source, local, stride, rest, most)
        return matmul(late, delivered(rows_of(table, late_ids))).astype(BF16)

    extra = lax.cond(most > CAPACITY, fetch_rest, lambda: jnp.zeros((slots, width), BF16))
    edge_out, mesh_out, copies = processor(
        place,
        live,
        got,
        extra,
        mesh_edges,
        mesh_latent,
        weight(table, 0, 12),
        weight(table, 12, 4),
        table.reshape(-1, stride, width),
        nodes + 16,
        weight(table, 24, 4),
        2 * group,
    )

    late_table, _ = lax.optimization_barrier((table, mesh_out))
    near = two_patches(copies)
    far = swapped(matmul(one_hot(outside, near.shape[0]), near).astype(BF16), "wide", 1)
    de_first = weight(late_table, 32, 12)
    first = decoder_first(named, index, near, decoder_edges, grid_latent, de_first)
    grid_pred = decoder_second(
        start,
        index,
        far,
        first,
        decoder_edges,
        grid_latent,
        de_first,
        weight(late_table, 44, 4),
        late_table.reshape(-1, stride, width),
        nodes + 48,
        weight(late_table, 56, 4),
        weight(late_table, 28, 4)[:, :channels],
    ).T
    return (mesh_out, edge_out, grid_pred)


def solution(mesh):
    rows = P(("wide", "narrow"), None)
    lists = P("wide", "narrow", None, None)
    return jax.shard_map(
        body,
        mesh=mesh,
        in_specs=(rows,) * 5 + (P(("wide", "narrow")), rows, lists, lists) + (P("wide", None),) * 9,
        out_specs=(rows,) * 3,
        check_vma=False,
    )
```

```python
import jax
import jax.numpy as jnp
from jax import lax
from jax.experimental import pallas as pl
from jax.experimental.pallas import tpu as pltpu
from jax.sharding import PartitionSpec as P

BF16 = jnp.bfloat16
F32 = jnp.float32
CAPACITY = 176


def matmul(a, b):
    return jnp.dot(a, b, preferred_element_type=F32)


def second_layer(pre, w_second):
    active = (pre / (1.0 + jnp.exp(-pre))).astype(BF16)
    values = matmul(active, w_second)
    center = values - jnp.mean(values, axis=-1, keepdims=True)
    spread = jnp.mean(center * center, axis=-1, keepdims=True)
    return center * lax.rsqrt(spread + 1e-05)


def marks(hit):
    return jnp.where(hit, 1.0, 0.0).astype(BF16)


def selection(index, size):
    columns = lax.broadcasted_iota(jnp.int32, (index.shape[0], size), 1)
    return marks(index == columns)


def pack_kernel(*refs):
    *pieces, out, stage = refs
    stage[...] = jnp.zeros_like(stage)
    first = 0
    for piece in pieces:
        rows, columns = piece.shape
        stage[first : first + rows, 0:columns] = piece[...].astype(F32)
        first += rows
    out[...] = stage[...].astype(BF16)


def packed(pieces, rows, width):
    return pl.pallas_call(
        pack_kernel,
        out_shape=jax.ShapeDtypeStruct((rows, width), BF16),
        scratch_shapes=[pltpu.VMEM((rows, width), F32)],
        name="pack",
    )(*pieces)


def rows_in(gathered, first, rows):
    shards, _, width = gathered.shape
    count = rows // shards
    return pl.BlockSpec((shards, count, width), lambda *_: (0, first // count, 0))


def keep_kernel(*refs):
    half = len(refs) // 2
    for source, target in zip(refs[:half], refs[half:]):
        target[...] = source[...]


def kept(columns):
    return pl.pallas_call(
        keep_kernel,
        out_shape=[jax.ShapeDtypeStruct(c.shape, c.dtype) for c in columns],
        name="columns",
    )(*columns)


def processor_kernel(
    place, live, got, extra, edges, near, latent, w_first, w_second, n_first, n_second, edge_out, mesh_out, copies, messages
):
    step, steps = pl.program_id(0), pl.num_programs(0)
    width = edges.shape[1]
    rows = matmul(selection(place[...], got.shape[0]), got[...]) + extra[...].astype(F32)
    sent = matmul(rows.astype(BF16), w_first[width : 2 * width]).astype(BF16)
    receiver = matmul(near[...], w_first[2 * width :])
    count = receiver.shape[0]
    spread = jnp.broadcast_to(receiver[:, None, :], (count, edges.shape[0] // count, width))
    pre = matmul(edges[...], w_first[:width]) + sent.astype(F32) + spread.reshape(edges.shape)
    updated = (edges[...].astype(F32) + second_layer(pre, w_second[...])).astype(BF16)
    edge_out[...] = updated
    kept = (updated.astype(F32) * live[...]).reshape(spread.shape)
    messages[pl.ds(pl.multiple_of(step * count, count), count)] = jnp.sum(kept, axis=1).astype(BF16)

    @pl.when(step == steps - 1)
    def _():
        inner = n_first[...].reshape(2 * width, width)
        node_pre = matmul(latent[...], inner[:width]) + matmul(messages[...], inner[width:])
        new = (latent[...].astype(F32) + second_layer(node_pre, n_second[...])).astype(BF16)
        mesh_out[...] = new
        for copy in range(copies.shape[0]):
            copies[copy] = new


def processor(place, live, got, extra, edges, latent, w_first, w_second, n_first, n_at, n_second, count, steps=2):
    slots, width = edges.shape
    nodes = latent.shape[0]

    def tiles(array):
        return pl.BlockSpec((array.shape[0] // steps, array.shape[1]), lambda i: (i, 0))

    def whole(array):
        return pl.BlockSpec(array.shape, lambda i: (0, 0))

    return pl.pallas_call(
        processor_kernel,
        grid=(steps,),
        in_specs=[tiles(place), tiles(live), whole(got), tiles(extra), tiles(edges), tiles(latent), whole(latent)]
        + [whole(w_first), whole(w_second), rows_in(n_first, n_at, 2 * width), whole(n_second)],
        out_specs=[tiles(edges), whole(latent), pl.BlockSpec((count, *latent.shape), lambda i: (0, 0, 0))],
        out_shape=[jax.ShapeDtypeStruct(a, BF16) for a in (edges.shape, latent.shape, (count, *latent.shape))],
        scratch_shapes=[pltpu.VMEM((nodes, width), BF16)],
        cost_estimate=pl.CostEstimate(flops=2_000_000_000, bytes_accessed=8_000_000, transcendentals=600_000),
        name="processor",
    )(place, live, got, extra, edges, latent, latent, w_first, w_second, n_first, n_second)


def decoder_first_kernel(named, index, near, edges, latent, w_first, out, sent):
    width = edges.shape[1]

    @pl.when(pl.program_id(0) == 0)
    def _():
        table = matmul(selection(named[...], near.shape[0]), near[...])
        sent[...] = matmul(table.astype(BF16), w_first[width : 2 * width]).astype(BF16)

    count, points = edges.shape[0], latent.shape[0]
    fanin = count // points
    offset = lax.broadcasted_iota(jnp.int32, (count, points), 0) - fanin * lax.broadcasted_iota(
        jnp.int32, (count, points), 1
    )
    receivers = matmul(marks((offset >= 0) & (offset < fanin)), latent[...]).astype(BF16)
    pre = matmul(edges[...], w_first[:width]) + matmul(receivers, w_first[2 * width :])
    out[...] = pre + matmul(selection(index[...], sent.shape[0]), sent[...])


def tiles_of(array, steps):
    return pl.BlockSpec((array.shape[0] // steps, array.shape[1]), lambda i: (i, 0))


def whole_of(array):
    return pl.BlockSpec(array.shape, lambda i: (0, 0))


def decoder_first(named, index, near, edges, latent, w_first, steps=2):
    out = jax.ShapeDtypeStruct(edges.shape, F32)
    return pl.pallas_call(
        decoder_first_kernel,
        grid=(steps,),
        in_specs=[
            whole_of(named),
            tiles_of(index, steps),
            whole_of(near),
            tiles_of(edges, steps),
            tiles_of(latent, steps),
            whole_of(w_first),
        ],
        out_specs=tiles_of(out, steps),
        out_shape=out,
        scratch_shapes=[pltpu.VMEM((named.shape[0], edges.shape[1]), BF16)],
        cost_estimate=pl.CostEstimate(flops=2_000_000_000, bytes_accessed=6_000_000, transcendentals=0),
        name="decoder_first",
    )(named, index, near, edges, latent, w_first)


def decoder_second_kernel(
    start, index, far, first, edges, latent, w_send, w_second, n_first, n_second, head, out
):
    count, width = edges.shape
    points = latent.shape[0]
    fanin = count // points
    onto = lax.broadcasted_iota(jnp.int32, (points, count), 1) - fanin * lax.broadcasted_iota(
        jnp.int32, (points, count), 0
    )
    sent = matmul(far[...], w_send[...]).astype(BF16)
    pre = first[...] + matmul(selection(index[...] - start[0], sent.shape[0]), sent)
    updated = (edges[...].astype(F32) + second_layer(pre, w_second[...])).astype(BF16)
    summed = matmul(marks((onto >= 0) & (onto < fanin)), updated).astype(BF16)
    inner = n_first[...].reshape(2 * width, width)
    point_pre = matmul(latent[...], inner[:width]) + matmul(summed, inner[width:])
    point_new = (latent[...].astype(F32) + second_layer(point_pre, n_second[...])).astype(BF16)
    out[...] = lax.dot_general(
        head[...], point_new, (((0,), (1,)), ((), ())), preferred_element_type=F32
    )


def decoder_second(start, index, far, first, edges, latent, w_first, w_second, n_first, n_at, n_second, head, steps=2):
    points, width = latent.shape
    channels = head.shape[1]
    send = pl.BlockSpec((width, width), lambda i: (1, 0))
    return pl.pallas_call(
        decoder_second_kernel,
        grid=(steps,),
        in_specs=[
            pl.BlockSpec(memory_space=pltpu.SMEM),
            tiles_of(index, steps),
            whole_of(far),
            tiles_of(first, steps),
            tiles_of(edges, steps),
            tiles_of(latent, steps),
            send,
        ]
        + [whole_of(w_second), rows_in(n_first, n_at, 2 * width), whole_of(n_second), whole_of(head)],
        out_specs=pl.BlockSpec((channels, points // steps), lambda i: (0, i)),
        out_shape=jax.ShapeDtypeStruct((channels, points), F32),
        cost_estimate=pl.CostEstimate(flops=2_000_000_000, bytes_accessed=6_000_000, transcendentals=1_000_000),
        name="decoder_second",
    )(start, index, far, first, edges, latent, w_first, w_second, n_first, n_second, head)


def exchanged(blocks, axis):
    return lax.all_to_all(blocks, axis, split_axis=0, concat_axis=0, tiled=True)


def swapped(block, axis, first):
    count = lax.axis_size(axis)
    pairs = [((first + i) % count, (first + (i ^ 1)) % count) for i in range(count)]
    return lax.ppermute(block, axis, pairs)


def one_hot(index, size):
    return (index[:, None] == lax.broadcasted_iota(jnp.int32, (1, size), 1)).astype(BF16)


def wanted_rows(senders, send_rows, nodes):
    peers, send = send_rows.shape
    group = lax.axis_size("narrow")
    patch = nodes * group
    slots = senders.reshape(-1)
    incoming = exchanged(send_rows, "wide")
    halo = jnp.maximum(slots - patch, 0)
    lists = matmul(one_hot(halo // send, peers), incoming.astype(BF16))
    column = lax.broadcasted_iota(jnp.int32, (1, send), 1)
    remote = jnp.sum(jnp.where((halo % send)[:, None] == column, lists, 0.0), axis=1)
    own = slots < patch
    row = jnp.where(own, slots, remote.astype(jnp.int32))
    source = jnp.where(own, lax.axis_index("wide"), halo // send)
    return row // nodes, source, row % nodes


def ranks_within(owner, group):
    mine = one_hot(owner, group)
    count = owner.shape[0]
    before = lax.broadcasted_iota(jnp.int32, (count, count), 0) > lax.broadcasted_iota(
        jnp.int32, (count, count), 1
    )
    earlier = matmul(before.astype(BF16), mine)
    rank = jnp.sum(earlier * mine.astype(F32), axis=1).astype(jnp.int32)
    most = jnp.max(jnp.sum(mine.astype(F32), axis=0))
    return rank, most


def requests(select, source, local, stride, capacity, most):
    group = lax.axis_size("narrow")
    asked = matmul(jnp.stack([source, local], axis=0).astype(BF16), select).astype(jnp.int32)
    ids = (asked[0] * stride + asked[1]).reshape(group, capacity)
    ids = jnp.pad(ids, ((0, 0), (0, -capacity % 128 + 128)))
    lane = lax.broadcasted_iota(jnp.int32, (1, ids.shape[1]), 1)
    here = exchanged(jnp.where(lane == capacity, most, ids), "narrow")
    return here[:, :capacity].reshape(-1), jnp.max(here[:, capacity])


def places(owner, rank, first, capacity):
    here = rank - first
    return jnp.where((here >= 0) & (here < capacity), owner * capacity + here, -1)


def rows_of(table, ids):
    return table.at[ids].get(mode="promise_in_bounds")


def delivered(found):
    width = found.shape[1]
    return exchanged(found.reshape(lax.axis_size("narrow"), -1, width), "narrow").reshape(-1, width)


def all_devices_max(value):
    copies = jnp.broadcast_to(value, (lax.axis_size("wide"), 8))
    return jnp.max(exchanged(copies, "wide"))


def two_patches(copies):
    group = copies.shape[0]
    count = lax.axis_size("narrow") * lax.axis_size("wide")
    members = [list(range(first, first + group)) for first in range(0, count, group)]
    got = lax.all_to_all(
        copies, ("wide", "narrow"), split_axis=0, concat_axis=0, axis_index_groups=members, tiled=True
    )
    return got.reshape(-1, copies.shape[2])


def body(
    mesh_latent,
    mesh_edges,
    grid_latent,
    decoder_edges,
    mesh_senders,
    mesh_degree,
    decoder_senders,
    mesh_send_rows,
    decoder_send_rows,
    proc_edge_in,
    proc_edge_out,
    proc_node_in,
    proc_node_out,
    dec_edge_in,
    dec_edge_out,
    grid_node_in,
    grid_node_out,
    output_head,
):
    nodes, width = mesh_latent.shape
    degree = mesh_senders.shape[1]
    slots = nodes * degree
    channels = output_head.shape[1]
    pieces = (mesh_latent, proc_edge_in, proc_edge_out, proc_node_in, proc_node_out, output_head)
    pieces = pieces + (dec_edge_in, dec_edge_out, grid_node_in, grid_node_out)
    pack = packed(pieces, 2 * nodes, width)
    stride = pack.shape[0]
    table = lax.all_gather(pack, "wide", axis=0, tiled=True)

    def weight(gathered, first, count):
        parts = gathered.reshape(-1, stride, width)
        return parts[:, nodes + first : nodes + first + count].reshape(-1, width)

    owner, source, local = wanted_rows(mesh_senders, mesh_send_rows[0, 0], nodes)
    rank, most = ranks_within(owner, lax.axis_size("narrow"))
    group = lax.axis_size("narrow")
    place = places(owner, rank, 0, CAPACITY)
    ids, most = requests(one_hot(place, group * CAPACITY), source, local, stride, CAPACITY, most.astype(jnp.int32))
    most = all_devices_max(most)
    lists = decoder_send_rows[0, 0]
    odd = lax.axis_index("wide") % 2
    span = nodes * group
    after, before = lists[0], lists[1]
    beside = swapped(jnp.where(odd == 1, before, after), "wide", 0) + (1 - odd) * span
    outside = jnp.where(odd == 1, after, before) + odd * span
    own = odd * span + jnp.arange(span, dtype=jnp.int32)
    nowhere = jnp.full(beside.shape, -1, jnp.int32)
    named = jnp.concatenate(
        [own, jnp.where(odd == 1, beside, nowhere), jnp.where(odd == 1, nowhere, beside)]
    )
    start = (span + odd * beside.shape[0]).reshape(1)
    live = lax.broadcasted_iota(jnp.int32, (nodes, degree), 1) < mesh_degree[:, None]
    columns = (
        place.reshape(-1, 1),
        live.astype(F32).reshape(-1, 1),
        named.reshape(-1, 1),
        decoder_senders.reshape(-1, 1),
    )
    columns, outside, start, ids = lax.optimization_barrier((kept(columns), outside, start, ids))
    place, live, named, index = columns
    found = rows_of(table, ids)
    got = delivered(found)
    most, _ = lax.optimization_barrier((most, found))

    def fetch_rest():
        rest = slots - CAPACITY
        late = one_hot(places(owner, rank, CAPACITY, rest), group * rest)
        late_ids, _ = requests(late, source, local, stride, rest, most)
        return matmul(late, delivered(rows_of(table, late_ids))).astype(BF16)

    extra = lax.cond(most > CAPACITY, fetch_rest, lambda: jnp.zeros((slots, width), BF16))
    pe_first = weight(table, 0, 12)
    next_table, _ = lax.optimization_barrier((table, pe_first))
    got, de_first = lax.optimization_barrier((got, weight(next_table, 32, 12)))
    edge_out, mesh_out, copies = processor(
        place,
        live,
        got,
        extra,
        mesh_edges,
        mesh_latent,
        pe_first,
        weight(table, 12, 4),
        table.reshape(-1, stride, width),
        nodes + 16,
        weight(table, 24, 4),
        2 * group,
    )

    late_table, _ = lax.optimization_barrier((table, mesh_out))
    near = two_patches(copies)
    far = swapped(matmul(one_hot(outside, near.shape[0]), near).astype(BF16), "wide", 1)
    first = decoder_first(named, index, near, decoder_edges, grid_latent, de_first)
    grid_pred = decoder_second(
        start,
        index,
        far,
        first,
        decoder_edges,
        grid_latent,
        de_first,
        weight(late_table, 44, 4),
        late_table.reshape(-1, stride, width),
        nodes + 48,
        weight(late_table, 56, 4),
        weight(late_table, 28, 4)[:, :channels],
    ).T
    return (mesh_out, edge_out, grid_pred)


def solution(mesh):
    rows = P(("wide", "narrow"), None)
    lists = P("wide", "narrow", None, None)
    return jax.shard_map(
        body,
        mesh=mesh,
        in_specs=(rows,) * 5 + (P(("wide", "narrow")), rows, lists, lists) + (P("wide", None),) * 9,
        out_specs=(rows,) * 3,
        check_vma=False,
    )
```
